32 devices in a mesh: row: 8 (over z, y), col: 4 (over x, core).
Axes of the slice: x: 2, y: 2, z: 4, core: 2. Of those that a mesh axis runs over, the one named last changes fastest.
Arguments:
- field: float32 [512, 64, 8, 512], P('row', 'col'), may hold values from -6 to 6
- modes: int32 [3, 256], replicated, may hold values from 0 to 511, as said below
Outputs:
- spectrum: float32 [64, 512, 8, 512], P(None, 'col', None, 'row')
- localized: float32 [512, 512], replicated
The draws below stay inside these ranges and needn't reach their ends.
Inputs may be any that keep to these rules, and one draw needn't show every extreme that they name: `modes`: row 0 holds kx in 0 to 255, row 1 ky in 0 to 511, row 2 kz in 0 to 63; triples may repeat.
All inputs are finite; a program needn't handle non-finite values.
Results may differ from the reference program's by a relative error of at most 0.00013.
Values sent between devices are 32-bit elements; how exact they have to be, the bound alone decides.
No kernel may reach another device: no remote copies, remote signals or barrier semaphores. Data moves between devices by JAX's collectives and lax.ppermute only.
A program may use at most 192 MiB of HBM per device.

```python
import math
import jax
import jax.numpy as jnp
from jax import lax

NX = 512
NY = 512
NZ = 64
MEMBERS = 8
MODES = 256
REACH = 64


def draw_modes(key, part):
    first_key, second_key, third_key = jax.random.split(jax.random.fold_in(key, 7), 3)
    first = jax.random.randint(first_key, (MODES,), 0, NX // 2)
    second = jax.random.randint(second_key, (MODES,), 0, NY)
    third = jax.random.randint(third_key, (MODES,), 0, NZ)
    return jnp.stack([first, second, third]).astype(jnp.int32)


def steps_of(rng, shape, pieces, least, largest):
    loudness = 1.0
    for dim, parts in pieces:
        heights = jax.random.uniform(jax.random.fold_in(jax.random.fold_in(rng, 6), dim), (parts,), jnp.float32, least / len(pieces), largest / len(pieces))
        loudness = loudness * jnp.repeat(jnp.exp(heights), shape[dim] // parts).reshape((-1,) + (1,) * (len(shape) - 1 - dim))
    return loudness


def bell_draw(rng, extent, scale, reach, cuts=(), kind=jnp.bfloat16):
    entries = jax.random.normal(rng, extent, jnp.float32) * scale
    if len(cuts) > 0:
        entries = steps_of(rng, extent, cuts, -0.22, 0.18) * entries
    return jnp.clip(entries, min=-reach, max=reach).astype(kind)


def setup_inputs(seed: int = 0) -> dict:
    streams_of = jax.random.split(jax.random.key(seed), 3)
    return {
        "field": bell_draw(streams_of[0], (NY, NZ, MEMBERS, NX), 1.0, 6.0, ((0, 8), (1, 4)), jnp.float32),
        "modes": draw_modes(jax.random.fold_in(streams_of[2], 71), 0),
    }


def taper_of(modes):
    first = modes[0].astype(jnp.float32)
    second = jnp.where(modes[1] < NY // 2, modes[1], modes[1] - NY).astype(jnp.float32)
    third = jnp.where(modes[2] < NZ // 2, modes[2], modes[2] - NZ).astype(jnp.float32)
    first = jnp.concatenate([first, first])
    second = jnp.concatenate([second, second])
    third = jnp.concatenate([third, third])
    dist = (first[:, None] - first[None, :]) ** 2 + (second[:, None] - second[None, :]) ** 2
    dist = dist + (third[:, None] - third[None, :]) ** 2
    return jnp.exp(-dist / (2.0 * REACH * REACH))

def covariance_of(coef, modes):
    anomaly = coef - lax.optimization_barrier(jnp.mean(coef, axis=0, keepdims=True))
    cov = jnp.dot(anomaly.T, anomaly, precision=lax.Precision.HIGHEST) / (MEMBERS - 1)
    return cov * taper_of(modes)

def reference(field, modes):
    factor = 1.0 / math.sqrt(NX * NY * NZ)

    def one_member(member):
        whole = jnp.fft.fftn(member)[:, :, :NX // 2] * factor
        whole = jnp.transpose(whole, (1, 0, 2))
        paired = jnp.stack([jnp.real(whole), jnp.imag(whole)], axis=-1)
        return paired.reshape(NZ, NY, NX).astype(jnp.float32)
    stacked = lax.map(one_member, jnp.transpose(field, (2, 0, 1, 3)))
    spectrum = jnp.transpose(stacked, (1, 2, 0, 3))
    real_rows = spectrum[modes[2], modes[1], :, 2 * modes[0]]
    imag_rows = spectrum[modes[2], modes[1], :, 2 * modes[0] + 1]
    coef = jnp.concatenate([real_rows.T, imag_rows.T], axis=1)
    return (spectrum, covariance_of(coef, modes))
```

```python
import functools
import math

import jax
import jax.numpy as jnp
from jax import lax
from jax.experimental import pallas as pl
from jax.experimental.pallas import tpu as pltpu
from jax.sharding import PartitionSpec as P

REACH = 64
LANES = 128
CHUNKS = 4


def tables(points, waves, length):
    phase = points[:, None] * waves[None, :] % length
    angle = phase.astype(jnp.float32) * (2.0 * math.pi / length)
    return (jnp.cos(angle), jnp.sin(angle))


def halves(table):
    high = lax.reduce_precision(table, 8, 7)
    return high.astype(jnp.bfloat16), (table - high).astype(jnp.bfloat16)


def split(value):
    high = value.astype(jnp.bfloat16)
    return high, (value - high.astype(jnp.float32)).astype(jnp.bfloat16)


def product(left, right):
    dot = functools.partial(jnp.dot, preferred_element_type=jnp.float32)
    return dot(left[0], right[0]) + (dot(left[0], right[1]) + dot(left[1], right[0]))


def rotated(value):
    width = value.shape[1]
    lane = lax.broadcasted_iota(jnp.int32, value.shape, 1)
    after = pltpu.roll(value, width - 1, 1)
    before = pltpu.roll(value, 1, 1)
    return jnp.where(lane % 2 == 0, after, -before)


def x_kernel(field_ref, high_ref, low_ref, out_ref):
    ny, _, members, width = field_ref.shape
    parts = out_ref.shape[0]
    wide = width // parts
    pack = LANES // wide
    value = jnp.swapaxes(field_ref[:, 0], 0, 1).reshape(members * ny, width)
    lines = product(split(value), (high_ref[...], low_ref[...]))
    for r in range(parts):
        for g in range(members // pack):
            out_ref[r, 0, :, g * LANES:(g + 1) * LANES] = jnp.concatenate(
                [
                    lines[m * ny:(m + 1) * ny, r * wide:(r + 1) * wide]
                    for m in range(g * pack, (g + 1) * pack)
                ],
                axis=1,
            )


def x_transform(field, high, low, parts, chunk, depth):
    ny, _, members, width = field.shape
    lanes = members * (width // parts)
    return pl.pallas_call(
        x_kernel,
        grid=(depth,),
        in_specs=[
            pl.BlockSpec((ny, 1, members, width), lambda i: (0, chunk * depth + i, 0, 0)),
            pl.BlockSpec((width, width), lambda i: (0, 0)),
            pl.BlockSpec((width, width), lambda i: (0, 0)),
        ],
        out_specs=pl.BlockSpec((parts, 1, ny, lanes), lambda i: (0, i, 0, 0)),
        out_shape=jax.ShapeDtypeStruct((parts, depth, ny, lanes), jnp.float32),
        name="x_transform",
    )(field, high, low)


def y_kernel(lines_ref, high_ref, low_ref, select_ref, *out_refs):
    parts, _, ny, lanes = lines_ref.shape
    value = lines_ref[...].reshape(parts * ny, lanes)
    both = jnp.concatenate([value, rotated(value)], axis=0)
    result = product((high_ref[...], low_ref[...]), split(both))
    for s, ref in enumerate(out_refs[:-1]):
        count = ref.shape[1]
        ref[0] = result[s * count:(s + 1) * count]
    high, low = split(result)
    dot = functools.partial(jnp.dot, preferred_element_type=jnp.float32)
    out_refs[-1][0] = dot(select_ref[...], high) + dot(select_ref[...], low)


def y_transform(lines, high, low, select, parts):
    sources, depth, ny, lanes = lines.shape
    length = sources * ny
    picks = select.shape[0]
    sizes = [length // parts] * parts + [picks]
    return pl.pallas_call(
        y_kernel,
        grid=(depth,),
        in_specs=[
            pl.BlockSpec((sources, 1, ny, lanes), lambda i: (0, i, 0, 0)),
            pl.BlockSpec((length, 2 * length), lambda i: (0, 0)),
            pl.BlockSpec((length, 2 * length), lambda i: (0, 0)),
            pl.BlockSpec((picks, length), lambda i: (0, 0)),
        ],
        out_specs=[pl.BlockSpec((1, n, lanes), lambda i: (i, 0, 0)) for n in sizes],
        out_shape=[jax.ShapeDtypeStruct((depth, n, lanes), jnp.float32) for n in sizes],
        name="y_transform",
    )(lines, high, low, select)


def z_kernel(*refs):
    level_refs, high_ref, low_ref, out_ref = refs[:-3], refs[-3], refs[-2], refs[-1]
    nz, block, members, wide = out_ref.shape
    lanes = members * wide
    stacked = jnp.concatenate([ref[...].reshape(-1, block, lanes) for ref in level_refs], axis=0)
    turned = jnp.swapaxes(stacked, 0, 1)
    for k in range(block):
        value = turned[k]
        both = jnp.concatenate([value, rotated(value)], axis=0)
        result = product((high_ref[...], low_ref[...]), split(both))
        parts = jnp.stack([result[:, m * wide:(m + 1) * wide] for m in range(members)])
        out_ref[:, k] = jnp.swapaxes(parts, 0, 1)


def z_transform(levels, high, low, members):
    depth, ny, lanes = levels[0].shape
    nz = high.shape[0]
    wide = lanes // members
    block = 8
    return pl.pallas_call(
        z_kernel,
        grid=(ny // block,),
        in_specs=[pl.BlockSpec((depth, block, lanes), lambda i: (0, i, 0)) for _ in levels]
        + [pl.BlockSpec((nz, 2 * nz), lambda i: (0, 0)) for _ in range(2)],
        out_specs=pl.BlockSpec((nz, block, members, wide), lambda i: (0, i, 0, 0)),
        out_shape=jax.ShapeDtypeStruct((nz, ny, members, wide), jnp.float32),
        name="z_transform",
    )(*levels, high, low)


def taper_of(modes, size_y, size_z, reach):
    first = modes[0].astype(jnp.float32)
    second = jnp.where(modes[1] < size_y // 2, modes[1], modes[1] - size_y).astype(jnp.float32)
    third = jnp.where(modes[2] < size_z // 2, modes[2], modes[2] - size_z).astype(jnp.float32)
    first = jnp.concatenate([first, first])
    second = jnp.concatenate([second, second])
    third = jnp.concatenate([third, third])
    dist = (first[:, None] - first[None, :]) ** 2 + (second[:, None] - second[None, :]) ** 2
    dist = dist + (third[:, None] - third[None, :]) ** 2
    return jnp.exp(-dist / (2.0 * reach * reach))


def per_device(field, modes, rows, cols):
    local_y, local_z, members, width = field.shape
    size_y = local_y * rows
    size_z = local_z * cols
    chunks = math.gcd(CHUNKS, local_z)
    depth = local_z // chunks
    local_q = width // rows
    local_k = size_y // cols
    factor = 1.0 / math.sqrt(width * size_y * size_z)

    points = lax.iota(jnp.int32, width)
    cos_x, sin_x = tables(points, lax.iota(jnp.int32, width) // 2, width)
    x_high, x_low = halves(jnp.where(points[None, :] % 2 == 0, cos_x, -sin_x))
    row = lax.axis_index("row")
    col = lax.axis_index("col")
    ahead = (col + lax.iota(jnp.int32, cols)) % cols
    behind = (col - lax.iota(jnp.int32, cols)) % cols
    lines_y = (ahead[:, None] * local_k + lax.iota(jnp.int32, local_k)[None, :]).reshape(-1)
    cos_y, sin_y = tables(lines_y, lax.iota(jnp.int32, size_y), size_y)
    y_high, y_low = halves(jnp.concatenate([cos_y, sin_y], axis=1))
    select = (lines_y[None, :] == modes[1][:, None]).astype(jnp.bfloat16)
    order = (
        lax.iota(jnp.int32, chunks)[:, None, None] * depth
        + behind[None, :, None] * local_z
        + lax.iota(jnp.int32, depth)[None, None, :]
    ).reshape(-1)
    cos_z, sin_z = tables(lax.iota(jnp.int32, size_z), order, size_z)
    z_high, z_low = halves(jnp.concatenate([cos_z, sin_z], axis=1) * factor)

    target = 2 * modes[0] - row * local_q
    columns = lax.iota(jnp.int32, local_q)[None, :]
    choose = jnp.stack([columns == target[:, None], columns == target[:, None] + 1], axis=2)
    choose = choose.astype(jnp.float32)
    own_z = col * local_z + lax.iota(jnp.int32, local_z)

    sent = [x_transform(field, x_high, x_low, rows, c, depth) for c in range(min(2, chunks))]
    levels = []
    partial_value = jnp.zeros((members, 2 * modes.shape[1]), jnp.float32)
    for c in range(chunks):
        gathered = lax.all_to_all(sent[c], "row", split_axis=0, concat_axis=0, tiled=True)
        gathered, partial_value = lax.optimization_barrier((gathered, partial_value))
        *blocks, picked = y_transform(gathered, y_high, y_low, select, cols)
        levels.append(blocks[0])
        for s in range(1, cols):
            ring = [(i, (i + s) % cols) for i in range(cols)]
            levels.append(lax.ppermute(blocks[s], "col", ring))
        picked = picked.reshape(depth, -1, members, local_q)
        real = jnp.sum(picked * choose[None, :, None, :, 0], axis=3)
        imag = jnp.sum(picked * choose[None, :, None, :, 1], axis=3)
        cos_s, sin_s = tables(own_z[c * depth:(c + 1) * depth], modes[2], size_z)
        cos_s = cos_s[:, :, None] * factor
        sin_s = sin_s[:, :, None] * factor
        real_sum = jnp.sum(real * cos_s + imag * sin_s, axis=0)
        imag_sum = jnp.sum(imag * cos_s - real * sin_s, axis=0)
        partial_value = partial_value + jnp.concatenate([real_sum.T, imag_sum.T], axis=1)
        if c + 2 < chunks:
            last = levels[-cols:]
            field, partial_value, last = lax.optimization_barrier((field, partial_value, last))
            levels[-cols:] = last
            sent.append(x_transform(field, x_high, x_low, rows, c + 2, depth))
    coef = lax.psum(partial_value, ("row", "col"))
    spectrum = z_transform(levels, z_high, z_low, members)
    anomaly = coef - jnp.mean(coef, axis=0, keepdims=True)
    cov = jnp.dot(anomaly.T, anomaly, precision=lax.Precision.HIGHEST) / (members - 1)
    localized = cov * taper_of(modes, size_y, size_z, REACH)
    return (spectrum, localized)


def solution(mesh):
    placed = (P("row", "col", None, None), P())
    body = functools.partial(per_device, rows=mesh.shape["row"], cols=mesh.shape["col"])
    return jax.shard_map(
        body,
        mesh=mesh,
        in_specs=placed,
        out_specs=(P(None, "col", None, "row"), P()),
        check_vma=False,
    )
```
